128 devices in a mesh: grp: 4 (over z), dev: 32 (over x, y, core).
Axes of the slice: x: 4, y: 4, z: 4, core: 2. Of those that a mesh axis runs over, the one named last changes fastest.
Arguments:
- inv_factor: bfloat16 [512, 384, 384], P(('grp', 'dev')), may hold values from -8 to 8
- border: bfloat16 [512, 384, 2048], P(('grp', 'dev')), may hold values from -0.107910156 to 0.107910156
- block_rows: int32 [512], P(('grp', 'dev')), may hold values from 96 to 384
- live_count: int32 [128], P(('grp', 'dev')), may hold values from 1 to 4, as said below
- first_section: float32 [2048, 2048], P('dev'), may hold values from -6 to 6
Outputs:
- condensed: bfloat16 [512, 384, 2048], P(('grp', 'dev'))
- schur: float32 [2048, 2048], P('dev')
The draws below stay inside these ranges and needn't reach their ends.
Inputs may be any that keep to these rules, and one draw needn't show every extreme that they name: `live_count`: every device holds 1 to 4 live scenarios; at least one device holds 4.
All inputs are finite; a program needn't handle non-finite values.
Results may differ from the reference program's by a relative error of at most 0.001.
Values sent between devices are 32-bit elements; how exact they have to be, the bound alone decides.
A program may use at most 192 MiB of HBM per device.

```python
import jax
import jax.numpy as jnp
from jax import lax

NB = 384
NS = 2048
SLOT = 4
SCEN = 512
DEVICES = 128


def draw_inv_factor(key, part):
    key_off = jax.random.fold_in(key, 11)
    key_diag = jax.random.fold_in(key, 12)
    offdiag = jax.random.normal(key_off, (SCEN, NB, NB), jnp.float32) * (0.3 / NB ** 0.5)
    offdiag = jnp.clip(offdiag, -0.1, 0.1)
    diag_vals = jax.random.uniform(key_diag, (SCEN, NB), jnp.float32, 1.0, 1.9)
    matrix = offdiag + jnp.eye(NB, dtype=jnp.float32)[None] * diag_vals[:, :, None]
    return matrix.astype(jnp.bfloat16)


def draw_live_count(key, part):
    key_one = jax.random.fold_in(key, 21)
    key_two = jax.random.fold_in(key, 22)
    key_pick = jax.random.fold_in(key, 23)
    first_draw = jax.random.randint(key_one, (DEVICES,), 1, SLOT + 1)
    second_draw = jax.random.randint(key_two, (DEVICES,), 1, SLOT + 1)
    values = jnp.minimum(first_draw, second_draw)
    chosen = jax.random.randint(key_pick, (), 0, DEVICES)
    values = jnp.where(jnp.arange(DEVICES) == chosen, SLOT, values)
    return values.astype(jnp.int32)


def with_ends(array, own_key, smallest, top_value):
    longest = array.shape.index(max(array.shape))
    spots = []
    for shift in (0, 1):
        where = [jax.random.randint(jax.random.fold_in(own_key, axis), (), 0, length) for axis, length in enumerate(array.shape)]
        where[longest] = (where[longest] + shift) % array.shape[longest]
        spots.append(tuple(where))
    return array.at[spots[0]].set(smallest).at[spots[1]].set(top_value)


def block_scale(key, shape, cuts, least, top_value):
    level = 1.0
    for axis_at, parts in cuts:
        steps = jax.random.uniform(jax.random.fold_in(jax.random.fold_in(key, 6), axis_at), (parts,), jnp.float32, least / len(cuts), top_value / len(cuts))
        level = level * jnp.repeat(jnp.exp(steps), shape[axis_at] // parts).reshape((-1,) + (1,) * (len(shape) - 1 - axis_at))
    return level


def bell_draw(rng, extent, width, bound, pieces=(), kind=jnp.bfloat16):
    array = jax.random.normal(rng, extent, jnp.float32) * width
    if len(pieces) > 0:
        array = block_scale(rng, extent, pieces, -0.22, 0.18) * array
    return jnp.clip(array, min=-bound, max=bound).astype(kind)


def setup_inputs(seed: int = 0) -> dict:
    keys = jax.random.split(jax.random.key(seed), 6)
    inv_factor = draw_inv_factor(jax.random.fold_in(keys[5], 71), 0)
    border = bell_draw(keys[1], (SCEN, NB, NS), 0.018, 0.107910156, ((0, 128),))
    block_rows = with_ends(jax.random.randint(keys[2], (SCEN,), NB // 4, NB + 1), jax.random.fold_in(keys[2], 1), NB // 4, NB).astype(jnp.int32)
    live_count = draw_live_count(jax.random.fold_in(keys[5], 71), 0)
    first_section = bell_draw(keys[4], (NS, NS), 1.0, 6.0, ((0, 32),), jnp.float32)
    return {"inv_factor": inv_factor, "border": border, "block_rows": block_rows, "live_count": live_count, "first_section": first_section}


def reference(inv_factor, border, block_rows, live_count, first_section):
    owners = jnp.arange(SCEN, dtype=jnp.int32) // SLOT
    within = jnp.arange(SCEN, dtype=jnp.int32) % SLOT
    alive = within < live_count[owners]
    row_ids = jnp.arange(NB, dtype=jnp.int32)

    def one_slot(running, items):
        inverse, border_piece, rows_live, is_live = items
        keep = (row_ids < rows_live) & is_live
        masked = jnp.where(keep[:, None], inverse, jnp.zeros_like(inverse))

        def compute(running_in):
            product = jnp.dot(masked.astype(jnp.float32), border_piece.astype(jnp.float32),
                              precision=lax.Precision.HIGHEST).astype(jnp.bfloat16)
            wide = product.astype(jnp.float32)
            update = jnp.dot(wide.T, wide, precision=lax.Precision.HIGHEST)
            return running_in + update, product

        def skipped(running_in):
            return running_in, jnp.zeros((NB, NS), jnp.bfloat16)

        return lax.cond(is_live, compute, skipped, running)

    total, condensed = lax.scan(one_slot, jnp.zeros((NS, NS), jnp.float32),
                                (inv_factor, border, block_rows, alive))
    return condensed, first_section - total
```

```python
import functools

import jax
import jax.numpy as jnp
from jax import lax
from jax.experimental import pallas as pl
from jax.experimental.pallas import tpu as pltpu
from jax.sharding import PartitionSpec as P

MESH = pl.DeviceIdType.MESH
SIDE = 4
BLK = 128
PIECE = BLK // 2 // SIDE
WIDE = 384
PARTS = 3


def condense_kernel(live_ref, rows_ref, inv_ref, border_ref, out_ref):
    slot = pl.program_id(0)
    rows = jnp.where(slot < live_ref[0], rows_ref[slot], 0)
    inverse = inv_ref[0]
    ids = lax.broadcasted_iota(jnp.int32, inverse.shape, 0)
    masked = jnp.where(ids < rows, inverse, jnp.zeros_like(inverse))
    out_ref[0] = jnp.dot(masked, border_ref[0], preferred_element_type=jnp.float32).astype(out_ref.dtype)


def condense(live_count, block_rows, inv_factor, border):
    slots, order, width = border.shape
    tile = width // 2
    return pl.pallas_call(
        condense_kernel,
        grid_spec=pltpu.PrefetchScalarGridSpec(
            num_scalar_prefetch=2,
            grid=(slots, width // tile),
            in_specs=[
                pl.BlockSpec((1, order, order), lambda s, j, *_: (s, 0, 0)),
                pl.BlockSpec((1, order, tile), lambda s, j, *_: (s, 0, j)),
            ],
            out_specs=pl.BlockSpec((1, order, tile), lambda s, j, *_: (s, 0, j)),
        ),
        out_shape=jax.ShapeDtypeStruct(border.shape, border.dtype),
        name="condense",
    )(live_count, block_rows, inv_factor, border)


def assemble_kernel(
    cond_ref, first_ref, out_ref,
    c_buf, ct_buf, g_buf, r_buf,
    rel0, rel1, rel2, left0, left1, left2, right0, right1, right2,
    q_buf, q_rel, q_left, q_right, w_buf, w_rel, w_left, w_right,
    z_buf, x_buf, t_buf, e_buf,
    load_sem, send_sem, recv_sem, e_sem,
):
    dev = lax.axis_index("dev")
    z = lax.axis_index("grp")
    core = dev % 2
    pair = dev // 2
    x, y = pair // SIDE, pair % SIDE
    other = 1 - core

    def at(xx, yy, zz, cc):
        return (zz, (xx * SIDE + yy) * 2 + cc)

    def near(axis, step):
        s = SIDE + step
        if axis == "x":
            return at((x + s) % SIDE, y, z, core)
        if axis == "y":
            return at(x, (y + s) % SIDE, z, core)
        return at(x, y, (z + s) % SIDE, core)

    sent = []

    def remote(src, dst, target, arrival=None):
        n = len(sent)
        copy = pltpu.make_async_remote_copy(
            src_ref=src, dst_ref=dst, send_sem=send_sem.at[n],
            recv_sem=recv_sem.at[n] if arrival is None else arrival,
            device_id=target, device_id_type=MESH,
        )
        sent.append(copy)
        copy.start()
        return copy

    order_x = (0, 1, 2, 3)
    order_y = ((y + 2) % SIDE, (y + 1) % SIDE, (y + 3) % SIDE, y)
    order_z = ((z + 2) % SIDE, (z + 1) % SIDE, (z + 3) % SIDE, z)

    barrier = pltpu.get_barrier_semaphore()
    peers = [at(x, y, z, other), near("z", 1), near("z", -1)]
    for r in range(1, 2 * SIDE):
        for turn in (r, 4 * SIDE - r):
            peer = (pair + turn) % (SIDE * SIDE)
            for cc in range(2):
                peers.append((z, peer * 2 + cc))
    for peer in peers:
        pl.semaphore_signal(barrier, inc=1, device_id=peer, device_id_type=MESH)

    tiles = c_buf.shape[2] // (2 * BLK)
    first_tile = (2 * ((x + 2) % SIDE)) % tiles
    loads = []
    for n in range(tiles):
        cols = pl.ds(pl.multiple_of(((first_tile + n) % tiles) * 2 * BLK, 2 * BLK), 2 * BLK)
        copy = pltpu.make_async_copy(cond_ref.at[:, :, cols], c_buf.at[:, :, cols], load_sem.at[n])
        copy.start()
        loads.append(copy)

    depth = c_buf.shape[0] * c_buf.shape[1]

    def tile_of(n):
        cols = pl.ds(pl.multiple_of((n % tiles) * 2 * BLK, 2 * BLK), 2 * BLK)
        return c_buf[:, :, cols].reshape(depth, 2 * BLK)

    def gram(h, yh):
        xx = (x + (2, 1, 3, 0)[h]) % SIDE
        i = 2 * xx + yh
        ct_buf[...] = jnp.transpose(tile_of(i))
        for j in range(5):
            product = jnp.dot(ct_buf[...], tile_of(i + j), preferred_element_type=jnp.float32)
            for a in range(2):
                for b in range(2):
                    rel = 2 * j + b - a
                    if 0 <= rel <= 8:
                        block = product[a * BLK:(a + 1) * BLK, b * BLK:(b + 1) * BLK]
                        off = BLK * (rel % 3)
                        g_buf[:, h, rel // 3, 2 * yh + a, :, :, off:off + BLK] = block.reshape(2, SIDE, PIECE, BLK)

    mine = g_buf.at[core]
    swaps = {}
    stage = {}

    def swap(h, yh):
        half = pl.ds(2 * yh, 2)
        swaps[h, yh] = remote(g_buf.at[other, h, :, half], r_buf.at[h, yh], at(x, y, z, other))

    def join(h, yh):
        swaps[h, yh].wait_recv()
        half = pl.ds(2 * yh, 2)
        for k in range(PARTS):
            g_buf[core, h, k, half] = g_buf[core, h, k, half] + r_buf[h, yh, k]

    lo, hi = pl.ds(0, 2), pl.ds(2, 2)

    def launch(h):
        yo, yr, yl, _ = order_y
        zo, zr, zl, _ = order_z
        if h == 0:
            stage["r0"] = remote(mine.at[0, 0, lo], rel0.at[0], near("x", 1))
            stage["l0"] = remote(mine.at[0, 0, hi], rel0.at[1], near("x", -1))
        stage["r1", h] = remote(mine.at[h, 1, yo, lo], rel1.at[h, 0], near("y", 1))
        stage["l1", h] = remote(mine.at[h, 1, yo, hi], rel1.at[h, 1], near("y", -1))
        stage["r2", h] = remote(mine.at[h, 2, lo, zo], rel2.at[h, 0], near("z", 1))
        stage["l2", h] = remote(mine.at[h, 2, hi, zo], rel2.at[h, 1], near("z", -1))
        if h == 1:
            stage["p0r"] = remote(mine.at[1, 0, hi], left0.at[hi], near("x", 1))
        if h == 2:
            stage["p0l"] = remote(mine.at[2, 0, lo], right0.at[lo], near("x", -1))
        stage["p1r", h] = remote(mine.at[h, 1, yr, hi], left1.at[h, hi], near("y", 1))
        stage["p1l", h] = remote(mine.at[h, 1, yl, lo], right1.at[h, lo], near("y", -1))
        stage["p2r", h] = remote(mine.at[h, 2, hi, zr], left2.at[h, hi], near("z", 1))
        stage["p2l", h] = remote(mine.at[h, 2, lo, zl], right2.at[h, lo], near("z", -1))

    def pass_x(h):
        if h == 1:
            stage["r0"].wait_recv()
            g_buf[core, 1, 0, lo] = g_buf[core, 1, 0, lo] + rel0[0]
            stage["f0r"] = remote(mine.at[1, 0, lo], left0.at[lo], near("x", 1))
        if h == 2:
            stage["l0"].wait_recv()
            g_buf[core, 2, 0, hi] = g_buf[core, 2, 0, hi] + rel0[1]
            stage["f0l"] = remote(mine.at[2, 0, hi], right0.at[hi], near("x", -1))

    def pass_yz(h):
        _, yr, yl, _ = order_y
        _, zr, zl, _ = order_z
        stage["r1", h].wait_recv()
        g_buf[core, h, 1, yr, lo] = g_buf[core, h, 1, yr, lo] + rel1[h, 0]
        stage["f1r", h] = remote(mine.at[h, 1, yr, lo], left1.at[h, lo], near("y", 1))
        stage["l1", h].wait_recv()
        g_buf[core, h, 1, yl, hi] = g_buf[core, h, 1, yl, hi] + rel1[h, 1]
        stage["f1l", h] = remote(mine.at[h, 1, yl, hi], right1.at[h, hi], near("y", -1))
        stage["r2", h].wait_recv()
        g_buf[core, h, 2, lo, zr] = g_buf[core, h, 2, lo, zr] + rel2[h, 0]
        stage["f2r", h] = remote(mine.at[h, 2, lo, zr], left2.at[h, lo], near("z", 1))
        stage["l2", h].wait_recv()
        g_buf[core, h, 2, hi, zl] = g_buf[core, h, 2, hi, zl] + rel2[h, 1]
        stage["f2l", h] = remote(mine.at[h, 2, hi, zl], right2.at[h, hi], near("z", -1))

    for s in range(8):
        if s == 0:
            for copy in loads[:5]:
                copy.wait()
        elif s == 1:
            loads[5].wait()
        elif s == 2:
            for copy in loads[6:]:
                copy.wait()
        gram(s // 2, s % 2)
        if s == 0:
            pl.semaphore_wait(barrier, len(peers))
        swap(s // 2, s % 2)
        if s >= 1:
            join((s - 1) // 2, (s - 1) % 2)
            if s % 2 == 0:
                h = s // 2 - 1
                launch(h)
                pass_x(h)
                if h >= 1:
                    pass_yz(h - 1)
    join(3, 1)
    launch(3)
    pass_yz(2)
    pass_yz(3)

    for name in ("p0r", "f0r", "p0l", "f0l"):
        stage[name].wait_recv()
    for yy in range(SIDE):
        q_buf[0, yy] = g_buf[core, 3, 0, yy] + left0[yy] + right0[yy]
    for h in range(SIDE):
        for name in ("p1r", "f1r", "p1l", "f1l"):
            stage[name, h].wait_recv()
        for zz in range(SIDE):
            q_buf[1, zz, h] = g_buf[core, h, 1, y, zz] + left1[h, zz] + right1[h, zz]
    for h in range(SIDE):
        for name in ("p2r", "f2r", "p2l", "f2l"):
            stage[name, h].wait_recv()
        for yy in range(SIDE):
            q_buf[2, h, yy] = g_buf[core, h, 2, yy, z] + left2[h, yy] + right2[h, yy]

    axes2 = (("y", order_y), ("z", order_z), ("x", order_x))
    hops = {}
    for k, (axis, (opp, rgt, lft, own)) in enumerate(axes2):
        hops["r", k] = remote(q_buf.at[k, opp, lo], q_rel.at[k, 0], near(axis, 1))
        hops["l", k] = remote(q_buf.at[k, opp, hi], q_rel.at[k, 1], near(axis, -1))
    for k, (axis, (opp, rgt, lft, own)) in enumerate(axes2):
        hops["pr", k] = remote(q_buf.at[k, rgt, hi], q_left.at[k, hi], near(axis, 1))
        hops["pl", k] = remote(q_buf.at[k, lft, lo], q_right.at[k, lo], near(axis, -1))
    for k, (axis, (opp, rgt, lft, own)) in enumerate(axes2):
        hops["r", k].wait_recv()
        q_buf[k, rgt, lo] = q_buf[k, rgt, lo] + q_rel[k, 0]
        hops["fr", k] = remote(q_buf.at[k, rgt, lo], q_left.at[k, lo], near(axis, 1))
        hops["l", k].wait_recv()
        q_buf[k, lft, hi] = q_buf[k, lft, hi] + q_rel[k, 1]
        hops["fl", k] = remote(q_buf.at[k, lft, hi], q_right.at[k, hi], near(axis, -1))
    for k, (axis, (opp, rgt, lft, own)) in enumerate(axes2):
        for name in ("pr", "fr", "pl", "fl"):
            hops[name, k].wait_recv()
        w_buf[k] = q_buf[k, own] + q_left[k] + q_right[k]

    top, low = pl.ds(0, PIECE // 2), pl.ds(PIECE // 2, PIECE // 2)
    axes3 = (("z", order_z), ("x", order_x), ("y", order_y))
    hops = {}
    for k, (axis, (opp, rgt, lft, own)) in enumerate(axes3):
        hops["r", k] = remote(w_buf.at[k, opp, top], w_rel.at[k, 0], near(axis, 1))
        hops["l", k] = remote(w_buf.at[k, opp, low], w_rel.at[k, 1], near(axis, -1))
    for k, (axis, (opp, rgt, lft, own)) in enumerate(axes3):
        hops["pr", k] = remote(w_buf.at[k, rgt, low], w_left.at[k, low], near(axis, 1))
        hops["pl", k] = remote(w_buf.at[k, lft, top], w_right.at[k, top], near(axis, -1))
    for k, (axis, (opp, rgt, lft, own)) in enumerate(axes3):
        hops["r", k].wait_recv()
        w_buf[k, rgt, top] = w_buf[k, rgt, top] + w_rel[k, 0]
        hops["fr", k] = remote(w_buf.at[k, rgt, top], w_left.at[k, top], near(axis, 1))
        hops["l", k].wait_recv()
        w_buf[k, lft, low] = w_buf[k, lft, low] + w_rel[k, 1]
        hops["fl", k] = remote(w_buf.at[k, lft, low], w_right.at[k, low], near(axis, -1))
    for k, (axis, (opp, rgt, lft, own)) in enumerate(axes3):
        for name in ("pr", "fr", "pl", "fl"):
            hops[name, k].wait_recv()
        z_buf[0, k] = w_buf[k, own] + w_left[k] + w_right[k]

    ra = remote(z_buf.at[0, :, top], z_buf.at[1, :, top], near("z", 1))
    lb = remote(z_buf.at[0, :, low], z_buf.at[2, :, low], near("z", -1))
    rb = remote(z_buf.at[0, :, low], z_buf.at[1, :, low], near("z", 1))
    la = remote(z_buf.at[0, :, top], z_buf.at[2, :, top], near("z", -1))
    ra.wait_recv()
    fa = remote(z_buf.at[1, :, top], z_buf.at[3, :, top], near("z", 1))
    lb.wait_recv()
    fb = remote(z_buf.at[2, :, low], z_buf.at[3, :, low], near("z", -1))
    for copy in (rb, la, fa, fb):
        copy.wait_recv()
    for slot, turn in enumerate((0, 3, 1, 2)):
        rows = pl.ds(pl.multiple_of(((z + turn) % SIDE) * PIECE, PIECE), PIECE)
        for k in range(PARTS):
            x_buf[rows, k * WIDE:(k + 1) * WIDE] = z_buf[slot, k]

    for r in range(1, 2 * SIDE):
        block = x_buf[:, r * BLK:(r + 1) * BLK]
        both = jnp.concatenate([block, pltpu.roll(block, BLK - 32, 1)], axis=0)
        turned = jnp.transpose(both)
        peer = (pair + r) % (SIDE * SIDE)
        for cc in range(2):
            t_buf[r - 1, cc] = turned[64 * cc:64 * cc + 32]
        for cc in range(2):
            remote(t_buf.at[r - 1, cc], e_buf.at[r - 1, core], (z, peer * 2 + cc), e_sem.at[r - 1, core])
    for rel in range(9):
        cols = pl.ds(pl.multiple_of(((pair + rel) % (SIDE * SIDE)) * BLK, BLK), BLK)
        out_ref[:, cols] = first_ref[:, cols] - x_buf[:, rel * BLK:(rel + 1) * BLK]
    lane = lax.broadcasted_iota(jnp.int32, (32, BLK), 1)
    for r in range(1, 2 * SIDE):
        for cc in range(2):
            pltpu.make_async_remote_copy(
                src_ref=t_buf.at[r - 1, cc], dst_ref=e_buf.at[r - 1, cc], send_sem=send_sem.at[0],
                recv_sem=e_sem.at[r - 1, cc], device_id=at(x, y, z, other), device_id_type=MESH,
            ).wait_recv()
        one, two = e_buf[r - 1, 0], e_buf[r - 1, 1]
        upper = jnp.where(lane < 64, one, pltpu.roll(two, 64, 1))
        under = jnp.where(lane < 64, pltpu.roll(one, 64, 1), two)
        cols = pl.ds(pl.multiple_of(((pair + SIDE * SIDE - r) % (SIDE * SIDE)) * BLK, BLK), BLK)
        out_ref[0:32, cols] = first_ref[0:32, cols] - upper
        out_ref[32:64, cols] = first_ref[32:64, cols] - under

    for copy in sent:
        copy.wait_send()


def assemble(condensed, first_section):
    f32 = jnp.float32
    copies = 160

    def vmem(*shape):
        return pltpu.VMEM(shape, f32)

    s, r, w = SIDE, PIECE, WIDE
    return pl.pallas_call(
        assemble_kernel,
        out_shape=jax.ShapeDtypeStruct(first_section.shape, f32),
        in_specs=[pl.BlockSpec(memory_space=pl.ANY), pl.BlockSpec(memory_space=pltpu.VMEM)],
        out_specs=pl.BlockSpec(memory_space=pltpu.VMEM),
        scratch_shapes=[
            pltpu.VMEM(condensed.shape, condensed.dtype),
            pltpu.VMEM((2 * BLK, condensed.shape[0] * condensed.shape[1]), condensed.dtype),
            vmem(2, s, PARTS, s, s, r, w),
            vmem(s, 2, PARTS, 2, s, r, w),
            vmem(2, 2, s, r, w), vmem(s, 2, 2, r, w), vmem(s, 2, 2, r, w),
            vmem(s, s, r, w), vmem(s, s, r, w), vmem(s, s, r, w),
            vmem(s, s, r, w), vmem(s, s, r, w), vmem(s, s, r, w),
            vmem(PARTS, s, s, r, w), vmem(PARTS, 2, 2, r, w), vmem(PARTS, s, r, w), vmem(PARTS, s, r, w),
            vmem(PARTS, s, r, w), vmem(PARTS, 2, r // 2, w), vmem(PARTS, r, w), vmem(PARTS, r, w),
            vmem(4, PARTS, r, w), vmem(64, PARTS * w), vmem(7, 2, 32, BLK), vmem(7, 2, 32, BLK),
            pltpu.SemaphoreType.DMA((8,)),
            pltpu.SemaphoreType.DMA((copies,)),
            pltpu.SemaphoreType.DMA((copies,)),
            pltpu.SemaphoreType.DMA((7, 2)),
        ],
        compiler_params=pltpu.CompilerParams(
            collective_id=0, has_side_effects=True, vmem_limit_bytes=56 << 20
        ),
        name="assemble",
    )(condensed, first_section)


def body(inv_factor, border, block_rows, live_count, first_section):
    condensed = condense(live_count, block_rows, inv_factor, border)
    return condensed, assemble(condensed, first_section)


def solution(mesh):
    placed = (
        P(("grp", "dev"), None, None),
        P(("grp", "dev"), None, None),
        P(("grp", "dev")),
        P(("grp", "dev")),
        P("dev", None),
    )
    return jax.shard_map(
        body,
        mesh=mesh,
        in_specs=placed,
        out_specs=(P(("grp", "dev"), None, None), P("dev", None)),
        check_vma=False,
    )
```
